32 devices in a mesh: dp: 8 (over z, y), mp: 4 (over x, core).
Axes of the slice: x: 2, y: 2, z: 4, core: 2. Of those that a mesh axis runs over, the one named last changes fastest.
Arguments:
- pred_input: bfloat16 [512, 256, 384], P('dp'), may hold values from -6 to 6
- proj_weight: bfloat16 [384, 1280], P('dp', 'mp'), may hold values from -0.3125 to 0.3125
- proj_bias: float32 [1280], P('mp'), may hold values from -3 to 3
- targets: bfloat16 [512, 256, 1280], P('dp', None, 'mp'), may hold values from -6 to 6
- block_masks: int32 [512, 4, 256], P('dp'), may hold values from 0 to 1, as said below
Outputs:
- loss: float32 [], replicated
- clip_scale: float32 [], replicated
- grad_weight: float32 [384, 1280], P('dp', 'mp')
- grad_bias: float32 [1280], P('mp')
The draws below stay inside these ranges and needn't reach their ends.
Inputs may be any that keep to these rules, and one draw needn't show every extreme that they name: `block_masks`: each of an image's 4 target blocks is a nonempty rectangle of patches on the 16 x 16 grid (row-major patch order); blocks may intersect.
All inputs are finite; a program needn't handle non-finite values.
Results may differ from the reference program's by a relative error of at most 0.0003.
Values may be sent and summed in bfloat16 or wider, within the bound.
A program may use at most 192 MiB of HBM per device.

```python
import jax
import jax.numpy as jnp
from jax import lax

D = 1280
E = 384
GRID = 16
BLOCKS = 4
IMG_DEV = 64
PATCHES = 256
IMAGES = 512


def draw_block_masks(key, part):
    keys = jax.random.split(key, 4)
    lowest = max(1, GRID * 5 // 16)
    highest = GRID // 2 + 1
    heights = jax.random.randint(keys[0], (IMAGES, BLOCKS, 1), lowest, highest)
    widths = jax.random.randint(keys[1], (IMAGES, BLOCKS, 1), lowest, highest)
    top_raw = jax.random.randint(keys[2], (IMAGES, BLOCKS, 1), 0, 1 << 20)
    left_raw = jax.random.randint(keys[3], (IMAGES, BLOCKS, 1), 0, 1 << 20)
    top_row = top_raw % (GRID - heights + 1)
    left_col = left_raw % (GRID - widths + 1)
    places = jnp.arange(GRID * GRID, dtype=jnp.int32)
    row_of = (places // GRID)[None, None, :]
    col_of = (places % GRID)[None, None, :]
    inside = (row_of >= top_row) & (row_of < top_row + heights) & (col_of >= left_col) & (col_of < left_col + widths)
    return inside.astype(jnp.int32)


def shard_levels(own_key, dims, pieces, low, high):
    level = 1.0
    for axis_at, blocks in pieces:
        draws = jax.random.uniform(jax.random.fold_in(jax.random.fold_in(own_key, 6), axis_at), (blocks,), jnp.float32, low / len(pieces), high / len(pieces))
        level = level * jnp.repeat(jnp.exp(draws), dims[axis_at] // blocks).reshape((-1,) + (1,) * (len(dims) - 1 - axis_at))
    return level


def scatter_about(rng, shape, spread, bound, pieces=(), held_as=jnp.bfloat16):
    values = spread * jax.random.normal(rng, shape, jnp.float32)
    if pieces:
        values = values * shard_levels(rng, shape, pieces, -0.22, 0.18)
    return jnp.clip(values, -bound, bound).astype(held_as)


def setup_inputs(seed: int = 0) -> dict:
    key_list = jax.random.split(jax.random.key(seed), 6)
    return {
        "pred_input": scatter_about(key_list[0], (IMAGES, PATCHES, E), 1.0, 6.0, ((0, 8),)),
        "proj_weight": scatter_about(key_list[1], (E, D), E ** -0.5, 0.3125, ((0, 8), (1, 4))),
        "proj_bias": scatter_about(key_list[2], (D,), 0.5, 3.0, ((0, 4),), jnp.float32),
        "targets": scatter_about(key_list[3], (IMAGES, PATCHES, D), 1.0, 6.0, ((0, 8), (2, 4))),
        "block_masks": draw_block_masks(jax.random.fold_in(key_list[5], 71), 0),
    }


def reference(pred_input, proj_weight, proj_bias, targets, block_masks):
    groups = IMAGES // IMG_DEV
    inputs_grouped = pred_input.reshape(groups, IMG_DEV * PATCHES, E)
    targets_grouped = targets.reshape(groups, IMG_DEV * PATCHES, D)
    coverage_all = lax.optimization_barrier(jnp.sum(block_masks, axis=1)).astype(jnp.float32)
    coverage_grouped = coverage_all.reshape(groups, IMG_DEV * PATCHES, 1)

    def step(carry, batch):
        grad_acc, bias_acc, loss_acc, count_acc = carry
        inputs_here, targets_here, coverage = batch
        target_f = targets_here.astype(jnp.float32)
        mean_feat = lax.optimization_barrier(jnp.mean(target_f, axis=1, keepdims=True))
        centered = target_f - mean_feat
        variance = lax.optimization_barrier(jnp.mean(centered * centered, axis=1, keepdims=True))
        tnorm = centered / jnp.sqrt(variance + 1e-05)
        pred = jnp.dot(inputs_here, proj_weight, preferred_element_type=jnp.float32) + proj_bias
        differ = pred - tnorm
        magnitude = jnp.abs(differ)
        smooth = jnp.where(magnitude < 1.0, 0.5 * differ * differ, magnitude - 0.5)
        clipped = coverage * jnp.clip(differ, -1.0, 1.0)
        source = clipped.astype(jnp.bfloat16)
        grad_acc = grad_acc + lax.dot_general(inputs_here, source, (((0,), (0,)), ((), ())), preferred_element_type=jnp.float32)
        bias_acc = bias_acc + lax.optimization_barrier(jnp.sum(clipped, axis=0))
        loss_acc = loss_acc + jnp.sum(coverage * smooth)
        count_acc = count_acc + jnp.sum(coverage)
        return ((grad_acc, bias_acc, loss_acc, count_acc), None)
    start = (jnp.zeros((E, D), jnp.float32), jnp.zeros((D,), jnp.float32), jnp.zeros((), jnp.float32), jnp.zeros((), jnp.float32))
    (grad_acc, bias_acc, loss_acc, total), unused = lax.scan(step, start, (inputs_grouped, targets_grouped, coverage_grouped))
    grad_w = grad_acc / total
    grad_b = bias_acc / total
    norm = jnp.sqrt(jnp.sum(grad_w * grad_w) + jnp.sum(grad_b * grad_b))
    clip_scale = jnp.minimum(1.0, 1.0 / (norm + 1e-06))
    loss = loss_acc / total / D
    return (loss, clip_scale, clip_scale * grad_w, clip_scale * grad_b)
```

```python
import functools

import jax
import jax.numpy as jnp
from jax import lax
from jax.experimental import pallas as pl
from jax.experimental.pallas import tpu as pltpu
from jax.sharding import PartitionSpec as P

F32 = jnp.float32
BF16 = jnp.bfloat16
MESH = pl.DeviceIdType.MESH
LANES = 128
GROUP = 8
PAIR = 2
CHUNK = 16


def pad_to(n, m):
    return (n + m - 1) // m * m


def kernel(ndp, nmp, x_hbm, w_ref, b_ref, t_hbm, m_hbm,
           loss_ref, clip_ref, gw_ref, gb_ref,
           xv, tv, mv, wall, wfull, wt, bcol, brow, ssend, srecv, rbuf, mbuf, cbuf,
           pa, pb, sa, sb, acc, gacc, lacc, gsend, grecv, fsend, frecv,
           xsem, tsem, msem, wss, wrs, sss, srs, gss, grs, fss, frs):
    images, feat, patches = tv.shape
    width = xv.shape[1]
    rows = w_ref.shape[0]
    rows_pad = gsend.shape[1] - 8
    featp = acc.shape[0]
    groups = images // GROUP
    ntot = ndp * nmp
    dp, mp = lax.axis_index("dp"), lax.axis_index("mp")
    me = dp * nmp + mp
    feat_full = feat * nmp

    def t_copy(g):
        s = pl.ds(g * GROUP, GROUP)
        return pltpu.make_async_copy(t_hbm.at[s], tv.at[s], tsem.at[g])

    def x_copy(g):
        s = pl.ds(g * GROUP * patches, GROUP * patches)
        return pltpu.make_async_copy(x_hbm.at[s], xv.at[s], xsem.at[g])

    m_copy = pltpu.make_async_copy(m_hbm, mv, msem)

    barrier = pltpu.get_barrier_semaphore()

    def greet(o, _):
        d = lax.rem(me + o, ntot)
        pl.semaphore_signal(barrier, inc=1, device_id=(d // nmp, lax.rem(d, nmp)), device_id_type=MESH)
        return 0

    lax.fori_loop(1, ntot, greet, 0)
    m_copy.start()
    for g in range(groups):
        t_copy(g).start()
    for g in range(groups):
        x_copy(g).start()

    acc[...] = jnp.zeros_like(acc)
    gacc[...] = jnp.zeros_like(gacc)
    lacc[...] = jnp.zeros_like(lacc)
    sb[...] = jnp.zeros_like(sb)
    wfull[...] = jnp.zeros_like(wfull)
    brow[...] = jnp.zeros_like(brow)
    brow[0:1, :feat] = b_ref[...]
    bcol[...] = jnp.transpose(jnp.broadcast_to(brow[0:1, :], (LANES, featp)))

    pl.semaphore_wait(barrier, ntot - 1)

    def w_copy(o):
        return pltpu.make_async_remote_copy(
            src_ref=w_ref, dst_ref=wall.at[o - 1], send_sem=wss.at[o - 1], recv_sem=wrs.at[o - 1],
            device_id=(lax.rem(dp + o, ndp), mp), device_id_type=MESH)

    for o in range(1, ndp):
        w_copy(o).start()

    def s_copy(o, g):
        return pltpu.make_async_remote_copy(
            src_ref=ssend.at[g], dst_ref=srecv.at[o - 1, g],
            send_sem=sss.at[o - 1, g], recv_sem=srs.at[o - 1, g],
            device_id=(dp, lax.rem(mp + o, nmp)), device_id_type=MESH)

    m_copy.wait()

    def cover(g, _):
        block = [jnp.sum(mv[g * GROUP + j], axis=0, keepdims=True) for j in range(GROUP)]
        cbuf[pl.ds(pl.multiple_of(g * GROUP, GROUP), GROUP), :] = jnp.concatenate(block, axis=0).astype(F32)
        return 0

    lax.fori_loop(0, groups, cover, 0)

    def stats(g, _):
        t_copy(g).wait()

        sums, squares = [], []
        for j in range(GROUP):
            i = g * GROUP + j
            part = jnp.zeros((CHUNK, patches), F32)
            for c in range(0, feat, CHUNK):
                part = part + tv[i, c:c + CHUNK, :].astype(F32)
            total = jnp.sum(part, axis=0, keepdims=True)
            mean = total * (1.0 / feat)
            part = jnp.zeros((CHUNK, patches), F32)
            for c in range(0, feat, CHUNK):
                centred = tv[i, c:c + CHUNK, :].astype(F32) - mean
                part = part + centred * centred
            sums.append(total)
            squares.append(jnp.sum(part, axis=0, keepdims=True))
        ssend[g] = jnp.concatenate(sums + squares, axis=0)

        @pl.when(g > 0)
        def _():
            for o in range(1, nmp):
                s_copy(o, g - 1).start()

        return 0

    lax.fori_loop(0, groups, stats, 0)

    def place(owner_static, block):
        wfull[owner_static * rows:(owner_static + 1) * rows, :feat] = block.astype(F32)

    for o in range(1, ndp):
        w_copy(o).wait_recv()
    for o in range(1, nmp):
        s_copy(o, groups - 1).start()
    for k in range(ndp):
        slot = lax.rem(dp - k + ndp, ndp)
        other = wall[jnp.maximum(slot - 1, 0)].astype(F32)
        mine = w_ref[...].astype(F32)
        place(k, jnp.where(slot == 0, mine, other))
    wt[...] = jnp.transpose(wfull[...])[:feat].astype(BF16)

    def x_rows(k):
        n = PAIR * patches
        return xv[pl.ds(pl.multiple_of(k * n, n), n), :]

    def project(p_ref, k):
        p_ref[...] = lax.dot_general(wt[...], x_rows(k), (((1,), (1,)), ((), ())), preferred_element_type=F32)

    def gradient(s_ref, k):
        acc[:feat, :] += jnp.dot(s_ref[...], x_rows(k), preferred_element_type=F32)

    def pointwise(p_ref, s_ref, k):
        img = k * PAIR
        rs = [rbuf[pl.ds(img + g, 1), :] for g in range(PAIR)]
        ms = [mbuf[pl.ds(img + g, 1), :] for g in range(PAIR)]
        cs = [cbuf[pl.ds(img + g, 1), :] for g in range(PAIR)]
        loss = jnp.zeros((CHUNK, patches), F32)
        for c in range(0, feat, CHUNK):
            bias = bcol[c:c + CHUNK, :]
            bias = jnp.concatenate([bias] * (patches // LANES), axis=1)
            total = jnp.zeros((CHUNK, LANES), F32)
            for g in range(PAIR):
                cols = slice(g * patches, (g + 1) * patches)
                t = tv[img + g, c:c + CHUNK, :].astype(F32)
                differ = (p_ref[c:c + CHUNK, cols] + bias) + (ms[g] - t * rs[g])
                clipped = jnp.clip(differ, -1.0, 1.0)
                source = clipped * cs[g]
                loss = loss + source * (differ - 0.5 * clipped)
                for h in range(0, patches, LANES):
                    total = total + source[:, h:h + LANES]
                s_ref[c:c + CHUNK, cols] = source.astype(BF16)
            gacc[c:c + CHUNK, :] += total
        lacc[...] += loss

    x_copy(0).wait()
    project(pa, 0)
    steps = images // PAIR
    per_group = GROUP // PAIR

    def outer(g, _):
        @pl.when(g + 1 < groups)
        def _():
            x_copy(g + 1).wait()

        for o in range(1, nmp):
            s_copy(o, g).wait_recv()
        parts = [ssend[g]] + [srecv[o - 1, g] for o in range(1, nmp)]
        sums = [p[:GROUP] for p in parts]
        mean = functools.reduce(jnp.add, sums) * (1.0 / feat_full)
        var = functools.reduce(jnp.add, [p[GROUP:] for p in parts])
        for s in sums:
            gap = s * (1.0 / feat) - mean
            var = var + feat * (gap * gap)
        rstd = lax.rsqrt(var * (1.0 / feat_full) + 1e-05)
        here = pl.ds(pl.multiple_of(g * GROUP, GROUP), GROUP)
        rbuf[here, :] = rstd
        mbuf[here, :] = mean * rstd

        def inner(j, _):
            k = g * per_group + 2 * j
            pointwise(pa, sa, k)
            project(pb, k + 1)
            gradient(sb, jnp.maximum(k - 1, 0))
            pointwise(pb, sb, k + 1)
            project(pa, jnp.minimum(k + 2, steps - 1))
            gradient(sa, k)
            return 0

        lax.fori_loop(0, per_group // 2, inner, 0)
        return 0

    lax.fori_loop(0, groups, outer, 0)
    gradient(sb, steps - 1)

    bias_part = jnp.sum(jnp.transpose(gacc[...]), axis=0, keepdims=True)
    loss_part = jnp.sum(lacc[...], keepdims=True)
    count_part = jnp.sum(cbuf[...], keepdims=True)
    row_of = lax.broadcasted_iota(jnp.int32, (8, featp), 0)
    extra = jnp.where(row_of == 0, bias_part, jnp.where(row_of == 1, loss_part, count_part))
    full = jnp.transpose(acc[...])
    for k in range(ndp):
        gsend[k, :rows, :] = full[k * rows:(k + 1) * rows, :]
        gsend[k, rows_pad:, :] = extra

    def g_copy(o):
        to = lax.rem(dp + o, ndp)
        return pltpu.make_async_remote_copy(
            src_ref=gsend.at[to], dst_ref=grecv.at[o - 1],
            send_sem=gss.at[o - 1], recv_sem=grs.at[o - 1],
            device_id=(to, mp), device_id_type=MESH)

    for o in range(1, ndp):
        g_copy(o).start()
    grad = gsend[dp, :rows, :]
    sums = gsend[dp, rows_pad:, :]
    for o in range(1, ndp):
        g_copy(o).wait_recv()
        grad = grad + grecv[o - 1, :rows, :]
        sums = sums + grecv[o - 1, rows_pad:, :]
    bias_grad = sums[0:1, :]
    square = jnp.sum(grad * grad, keepdims=True)
    bias_square = jnp.sum(bias_grad * bias_grad, keepdims=True)
    row_of = lax.broadcasted_iota(jnp.int32, (8, LANES), 0)
    fsend[...] = jnp.where(row_of == 0, square + bias_square * (1.0 / ndp), sums[1:2, :LANES])

    def f_copy(o):
        d = lax.rem(me + o, ntot)
        return pltpu.make_async_remote_copy(
            src_ref=fsend, dst_ref=frecv.at[o - 1], send_sem=fss.at[o - 1], recv_sem=frs.at[o - 1],
            device_id=(d // nmp, lax.rem(d, nmp)), device_id_type=MESH)

    def f_start(o, _):
        f_copy(o).start()
        return 0

    def f_wait(o, _):
        f_copy(o).wait_recv()
        return 0

    lax.fori_loop(1, ntot, f_start, 0)
    count = sums[2:3, :LANES]
    lax.fori_loop(1, ntot, f_wait, 0)
    final = fsend[...] + jnp.sum(frecv[...], axis=0)
    norm = jnp.sqrt(final[0:1, :]) / count
    scale = jnp.minimum(1.0, 1.0 / (norm + 1e-06))
    factor = scale / count
    loss = final[1:2, :] / count * (1.0 / (feat_full * ndp))
    loss_ref[...] = loss
    clip_ref[...] = scale
    wide = jnp.concatenate([factor] * (featp // LANES), axis=1)
    gw_ref[...] = (grad * wide)[:, :feat]
    gb_ref[...] = (bias_grad * wide)[:, :feat]

    for o in range(1, ndp):
        w_copy(o).wait_send()
        g_copy(o).wait_send()

    def s_drain(g, _):
        for o in range(1, nmp):
            s_copy(o, g).wait_send()
        return 0

    def f_drain(o, _):
        f_copy(o).wait_send()
        return 0

    lax.fori_loop(0, groups, s_drain, 0)
    lax.fori_loop(1, ntot, f_drain, 0)


def body(pred_input, proj_weight, proj_bias, targets, block_masks):
    images, patches, width = pred_input.shape
    feat = targets.shape[2]
    rows = proj_weight.shape[0]
    blocks = block_masks.shape[1]
    ndp, nmp = lax.axis_size("dp"), lax.axis_size("mp")
    ntot = ndp * nmp
    featp = pad_to(feat, LANES)
    rows_pad = pad_to(rows, 8)
    groups = images // GROUP
    dma = pltpu.SemaphoreType.DMA
    vmem = pl.BlockSpec(memory_space=pltpu.VMEM)
    hbm = pl.BlockSpec(memory_space=pl.ANY)
    loss, clip, gw, gb = pl.pallas_call(
        functools.partial(kernel, ndp, nmp),
        out_shape=(
            jax.ShapeDtypeStruct((1, LANES), F32),
            jax.ShapeDtypeStruct((1, LANES), F32),
            jax.ShapeDtypeStruct((rows, feat), F32),
            jax.ShapeDtypeStruct((1, feat), F32),
        ),
        in_specs=[hbm, vmem, vmem, hbm, hbm],
        out_specs=(vmem,) * 4,
        scratch_shapes=[
            pltpu.VMEM((images * patches, width), BF16),
            pltpu.VMEM((images, feat, patches), BF16),
            pltpu.VMEM((images, blocks, patches), jnp.int32),
            pltpu.VMEM((ndp - 1, rows, feat), BF16),
            pltpu.VMEM((width, featp), F32),
            pltpu.VMEM((feat, width), BF16),
            pltpu.VMEM((featp, LANES), F32),
            pltpu.VMEM((8, featp), F32),
            pltpu.VMEM((groups, 2 * GROUP, patches), F32),
            pltpu.VMEM((nmp - 1, groups, 2 * GROUP, patches), F32),
            pltpu.VMEM((images, patches), F32),
            pltpu.VMEM((images, patches), F32),
            pltpu.VMEM((images, patches), F32),
            pltpu.VMEM((feat, PAIR * patches), F32),
            pltpu.VMEM((feat, PAIR * patches), F32),
            pltpu.VMEM((feat, PAIR * patches), BF16),
            pltpu.VMEM((feat, PAIR * patches), BF16),
            pltpu.VMEM((featp, width), F32),
            pltpu.VMEM((featp, LANES), F32),
            pltpu.VMEM((CHUNK, patches), F32),
            pltpu.VMEM((ndp, rows_pad + 8, featp), F32),
            pltpu.VMEM((ndp - 1, rows_pad + 8, featp), F32),
            pltpu.VMEM((8, LANES), F32),
            pltpu.VMEM((ntot - 1, 8, LANES), F32),
            dma((groups,)), dma((groups,)), dma(()),
            dma((ndp - 1,)), dma((ndp - 1,)),
            dma((nmp - 1, groups)), dma((nmp - 1, groups)),
            dma((ndp - 1,)), dma((ndp - 1,)),
            dma((ntot - 1,)), dma((ntot - 1,)),
        ],
        compiler_params=pltpu.CompilerParams(
            collective_id=0, has_side_effects=True, vmem_limit_bytes=60 * 1024 * 1024
        ),
    )(
        pred_input.reshape(images * patches, width),
        proj_weight,
        proj_bias.reshape(1, feat),
        jnp.swapaxes(targets, 1, 2),
        block_masks,
    )
    return loss[0, 0], clip[0, 0], gw, gb.reshape(feat)


def solution(mesh):
    in_specs = (
        P("dp", None, None),
        P("dp", "mp"),
        P("mp"),
        P("dp", None, "mp"),
        P("dp", None, None),
    )
    out_specs = (P(), P(), P("dp", "mp"), P("mp"))
    return jax.shard_map(body, mesh=mesh, in_specs=in_specs, out_specs=out_specs, check_vma=False)
```

```python
import functools

import jax
import jax.numpy as jnp
from jax import lax
from jax.experimental import pallas as pl
from jax.experimental.pallas import tpu as pltpu
from jax.sharding import PartitionSpec as P

F32 = jnp.float32
BF16 = jnp.bfloat16
MESH = pl.DeviceIdType.MESH
LANES = 128
GROUP = 8
PAIR = 2
CHUNK = 16


def pad_to(n, m):
    return (n + m - 1) // m * m


def layout(rows, feat):
    starts, at = [], 0
    for _ in range(feat // LANES):
        starts.append(at)
        at += pad_to(rows, 8)
    if feat % LANES:
        starts.append(at)
        at += pad_to(rows // 2, 8)
    starts.append(at)
    return starts, at + 8


def finish(ndp, nmp, sum_ref, fin_ref, loss_ref, clip_ref, gw_ref, gb_ref):
    rows, feat = gw_ref.shape
    starts, _ = layout(rows, feat)
    tiles = pad_to(feat, LANES) // LANES
    count = sum_ref[starts[-1] + tiles + 1:starts[-1] + tiles + 2, 0:1]
    square, loss = fin_ref[:, 0:1], fin_ref[:, 1:2]
    norm = jnp.sqrt(square) / count
    scale = jnp.minimum(1.0, 1.0 / (norm + 1e-06))
    factor = scale / count
    loss_ref[...] = loss / count * (1.0 / (feat * nmp * ndp))
    clip_ref[...] = scale
    for n in range(feat // LANES):
        gw_ref[:, n * LANES:(n + 1) * LANES] = sum_ref[starts[n]:starts[n] + rows, :] * factor
    half = LANES // 2
    if feat % LANES:
        packed = sum_ref[starts[-2]:starts[-2] + rows // 2, :] * factor
        gw_ref[:rows // 2, feat - half:] = packed[:, :half]
        gw_ref[rows // 2:, feat - half:] = packed[:, half:]
    for n in range(tiles):
        stop = min((n + 1) * LANES, feat)
        bias = sum_ref[starts[-1] + n:starts[-1] + n + 1, :] * factor
        gb_ref[:, n * LANES:stop] = bias[:, :stop - n * LANES]


def kernel(ndp, nmp, x_hbm, w_ref, b_ref, t_hbm, m_hbm,
           out_ref, fin_ref,
           xv, tv, mv, wall, wfull, wt, bcol, brow, ssend, srecv, rbuf, mbuf, cbuf,
           pa, pb, sa, sb, acc, gacc, lacc, gsend, pairv, gmid, grecv, fsend, frecv,
           xsem, tsem, msem, wss, wrs, sss, srs, pss, prs, gss, grs, fss, frs):
    images, feat, patches = tv.shape
    width = xv.shape[1]
    rows = w_ref.shape[0]
    dp, mp = lax.axis_index("dp"), lax.axis_index("mp")
    inner_dp = gsend.shape[0]
    outer_dp = gsend.shape[1]
    near, far = lax.rem(dp, inner_dp), dp // inner_dp
    featp = acc.shape[0]
    groups = images // GROUP
    ntot = ndp * nmp
    me = dp * nmp + mp
    feat_full = feat * nmp

    def t_copy(g):
        s = pl.ds(g * GROUP, GROUP)
        return pltpu.make_async_copy(t_hbm.at[s], tv.at[s], tsem.at[g])

    def x_copy(g):
        s = pl.ds(g * GROUP * patches, GROUP * patches)
        return pltpu.make_async_copy(x_hbm.at[s], xv.at[s], xsem.at[g])

    m_copy = pltpu.make_async_copy(m_hbm, mv, msem)

    barrier = pltpu.get_barrier_semaphore()

    def greet(o, _):
        d = lax.rem(me + o, ntot)
        pl.semaphore_signal(barrier, inc=1, device_id=(d // nmp, lax.rem(d, nmp)), device_id_type=MESH)
        return 0

    lax.fori_loop(1, ntot, greet, 0)
    m_copy.start()
    for g in range(groups):
        t_copy(g).start()
    acc[...] = jnp.zeros_like(acc)
    gacc[...] = jnp.zeros_like(gacc)
    lacc[...] = jnp.zeros_like(lacc)
    sb[...] = jnp.zeros_like(sb)
    wfull[...] = jnp.zeros_like(wfull)
    brow[...] = jnp.zeros_like(brow)
    brow[0:1, :feat] = b_ref[...]
    bcol[...] = jnp.transpose(jnp.broadcast_to(brow[0:1, :], (LANES, featp)))

    pl.semaphore_wait(barrier, ntot - 1)

    def w_copy(o):
        return pltpu.make_async_remote_copy(
            src_ref=w_ref, dst_ref=wall.at[o - 1], send_sem=wss.at[o - 1], recv_sem=wrs.at[o - 1],
            device_id=(lax.rem(dp + o, ndp), mp), device_id_type=MESH)

    for o in range(1, ndp):
        w_copy(o).start()

    def s_copy(o, g):
        return pltpu.make_async_remote_copy(
            src_ref=ssend.at[g], dst_ref=srecv.at[o - 1, g],
            send_sem=sss.at[o - 1, g], recv_sem=srs.at[o - 1, g],
            device_id=(dp, lax.rem(mp + o, nmp)), device_id_type=MESH)

    m_copy.wait()

    def cover(g, _):
        block = [jnp.sum(mv[g * GROUP + j], axis=0, keepdims=True) for j in range(GROUP)]
        cbuf[pl.ds(pl.multiple_of(g * GROUP, GROUP), GROUP), :] = jnp.concatenate(block, axis=0).astype(F32)
        return 0

    lax.fori_loop(0, groups, cover, 0)

    def stats(g, _):
        t_copy(g).wait()

        @pl.when(g >= 2)
        def _():
            x_copy(g - 2).start()

        sums, squares = [], []
        for j in range(GROUP):
            i = g * GROUP + j
            part = jnp.zeros((CHUNK, patches), F32)
            for c in range(0, feat, CHUNK):
                part = part + tv[i, c:c + CHUNK, :].astype(F32)
            total = jnp.sum(part, axis=0, keepdims=True)
            mean = total * (1.0 / feat)
            part = jnp.zeros((CHUNK, patches), F32)
            for c in range(0, feat, CHUNK):
                centred = tv[i, c:c + CHUNK, :].astype(F32) - mean
                part = part + centred * centred
            sums.append(total)
            squares.append(jnp.sum(part, axis=0, keepdims=True))
        ssend[g] = jnp.concatenate(sums + squares, axis=0)

        @pl.when(g > 0)
        def _():
            for o in range(1, nmp):
                s_copy(o, g - 1).start()

        return 0

    lax.fori_loop(0, groups, stats, 0)
    for g in range(groups - 2, groups):
        x_copy(g).start()

    def place(owner_static, block):
        wfull[owner_static * rows:(owner_static + 1) * rows, :feat] = block.astype(F32)

    for o in range(1, ndp):
        w_copy(o).wait_recv()
    for o in range(1, nmp):
        s_copy(o, groups - 1).start()
    for k in range(ndp):
        slot = lax.rem(dp - k + ndp, ndp)
        other = wall[jnp.maximum(slot - 1, 0)].astype(F32)
        mine = w_ref[...].astype(F32)
        place(k, jnp.where(slot == 0, mine, other))
    wt[...] = jnp.transpose(wfull[...])[:feat].astype(BF16)

    def x_rows(k):
        n = PAIR * patches
        return xv[pl.ds(pl.multiple_of(k * n, n), n), :]

    def project(p_ref, k):
        p_ref[...] = lax.dot_general(wt[...], x_rows(k), (((1,), (1,)), ((), ())), preferred_element_type=F32)

    def gradient(s_ref, k):
        acc[:feat, :] += jnp.dot(s_ref[...], x_rows(k), preferred_element_type=F32)

    def pointwise(p_ref, s_ref, k):
        img = k * PAIR
        rs = [rbuf[pl.ds(img + g, 1), :] for g in range(PAIR)]
        ms = [mbuf[pl.ds(img + g, 1), :] for g in range(PAIR)]
        cs = [cbuf[pl.ds(img + g, 1), :] for g in range(PAIR)]
        loss = jnp.zeros((CHUNK, patches), F32)
        for c in range(0, feat, CHUNK):
            bias = bcol[c:c + CHUNK, :]
            bias = jnp.concatenate([bias] * (patches // LANES), axis=1)
            total = jnp.zeros((CHUNK, LANES), F32)
            for g in range(PAIR):
                cols = slice(g * patches, (g + 1) * patches)
                t = tv[img + g, c:c + CHUNK, :].astype(F32)
                differ = (p_ref[c:c + CHUNK, cols] + bias) + (ms[g] - t * rs[g])
                clipped = jnp.clip(differ, -1.0, 1.0)
                source = clipped * cs[g]
                loss = loss + source * (differ - 0.5 * clipped)
                for h in range(0, patches, LANES):
                    total = total + source[:, h:h + LANES]
                s_ref[c:c + CHUNK, cols] = source.astype(BF16)
            gacc[c:c + CHUNK, :] += total
        lacc[...] += loss

    x_copy(0).wait()
    project(pa, 0)
    steps = images // PAIR
    per_group = GROUP // PAIR

    def outer(g, _):
        @pl.when(g + 1 < groups)
        def _():
            x_copy(g + 1).wait()

        for o in range(1, nmp):
            s_copy(o, g).wait_recv()
        parts = [ssend[g]] + [srecv[o - 1, g] for o in range(1, nmp)]
        sums = [p[:GROUP] for p in parts]
        mean = functools.reduce(jnp.add, sums) * (1.0 / feat_full)
        var = functools.reduce(jnp.add, [p[GROUP:] for p in parts])
        for s in sums:
            gap = s * (1.0 / feat) - mean
            var = var + feat * (gap * gap)
        rstd = lax.rsqrt(var * (1.0 / feat_full) + 1e-05)
        here = pl.ds(pl.multiple_of(g * GROUP, GROUP), GROUP)
        rbuf[here, :] = rstd
        mbuf[here, :] = mean * rstd

        def inner(j, _):
            k = g * per_group + 2 * j
            pointwise(pa, sa, k)
            project(pb, k + 1)
            gradient(sb, jnp.maximum(k - 1, 0))
            pointwise(pb, sb, k + 1)
            project(pa, jnp.minimum(k + 2, steps - 1))
            gradient(sa, k)
            return 0

        lax.fori_loop(0, per_group // 2, inner, 0)
        return 0

    lax.fori_loop(0, groups, outer, 0)
    gradient(sb, steps - 1)

    bias_part = jnp.sum(jnp.transpose(gacc[...]), axis=0, keepdims=True)
    loss_part = jnp.sum(lacc[...], keepdims=True)
    count_part = jnp.sum(cbuf[...], keepdims=True)
    at_row = lax.broadcasted_iota(jnp.int32, (8, LANES), 0)
    tiles = featp // LANES
    extra = jnp.where(at_row == tiles, loss_part, count_part)
    for n in range(tiles):
        extra = jnp.where(at_row == n, bias_part[:, n * LANES:(n + 1) * LANES], extra)
    starts, total_rows = layout(rows, feat)
    full = jnp.transpose(acc[...])
    for k in range(ndp):
        slot = gsend.at[k % inner_dp, k // inner_dp]
        if rows % 16:
            slot[...] = jnp.zeros(slot.shape, F32)
        mine = full[k * rows:(k + 1) * rows]
        for n in range(feat // LANES):
            slot[starts[n]:starts[n] + rows, :] = mine[:, n * LANES:(n + 1) * LANES]
        if feat % LANES:
            slot[starts[-2]:starts[-2] + rows // 2, :] = jnp.concatenate(
                [mine[:rows // 2, feat - LANES // 2:feat], mine[rows // 2:, feat - LANES // 2:feat]], axis=1)
        slot[starts[-1]:, :] = extra

    other = 1 - near

    def p_copy(o):
        to = lax.rem(far + o, outer_dp)
        return pltpu.make_async_remote_copy(
            src_ref=gsend.at[other, to], dst_ref=pairv.at[o], send_sem=pss.at[o], recv_sem=prs.at[o],
            device_id=(far * inner_dp + other, mp), device_id_type=MESH)

    def g_copy(o):
        to = lax.rem(far + o, outer_dp)
        return pltpu.make_async_remote_copy(
            src_ref=gmid.at[o - 1], dst_ref=grecv.at[o - 1], send_sem=gss.at[o - 1], recv_sem=grs.at[o - 1],
            device_id=(to * inner_dp + near, mp), device_id_type=MESH)

    order = list(range(1, outer_dp)) + [0]
    for o in order:
        p_copy(o).start()
    for o in order:
        p_copy(o).wait_recv()
        pair = gsend[near, lax.rem(far + o, outer_dp)] + pairv[o]
        if o:
            gmid[o - 1] = pair
            g_copy(o).start()
    for o in range(1, outer_dp):
        g_copy(o).wait_recv()
        pair = pair + grecv[o - 1]
    out_ref[...] = pair
    grad = pair[:starts[-1]]
    sums = pair[starts[-1]:]
    bias_grad = sums[:tiles]
    square = jnp.sum(grad * grad, keepdims=True)
    bias_square = jnp.sum(bias_grad * bias_grad, keepdims=True)
    lane = lax.broadcasted_iota(jnp.int32, (1, LANES), 1)
    fsend[...] = jnp.where(lane == 0, square + bias_square * (1.0 / ndp), sums[tiles:tiles + 1, :])

    def f_copy(o):
        d = lax.rem(me + o, ntot)
        return pltpu.make_async_remote_copy(
            src_ref=fsend, dst_ref=frecv.at[o - 1], send_sem=fss.at[o - 1], recv_sem=frs.at[o - 1],
            device_id=(d // nmp, lax.rem(d, nmp)), device_id_type=MESH)

    def f_start(o, _):
        f_copy(o).start()
        return 0

    def f_wait(o, _):
        f_copy(o).wait_recv()
        return 0

    lax.fori_loop(1, ntot, f_start, 0)
    lax.fori_loop(1, ntot, f_wait, 0)
    fin_ref[...] = fsend[...] + jnp.sum(frecv[...], axis=0)

    for o in range(1, ndp):
        w_copy(o).wait_send()
    for o in order:
        p_copy(o).wait_send()
        if o:
            g_copy(o).wait_send()

    def s_drain(g, _):
        for o in range(1, nmp):
            s_copy(o, g).wait_send()
        return 0

    def f_drain(o, _):
        f_copy(o).wait_send()
        return 0

    lax.fori_loop(0, groups, s_drain, 0)
    lax.fori_loop(1, ntot, f_drain, 0)


def body(pred_input, proj_weight, proj_bias, targets, block_masks):
    images, patches, width = pred_input.shape
    feat = targets.shape[2]
    rows = proj_weight.shape[0]
    blocks = block_masks.shape[1]
    ndp, nmp = lax.axis_size("dp"), lax.axis_size("mp")
    ntot = ndp * nmp
    featp = pad_to(feat, LANES)
    groups = images // GROUP
    dma = pltpu.SemaphoreType.DMA
    vmem = pl.BlockSpec(memory_space=pltpu.VMEM)
    hbm = pl.BlockSpec(memory_space=pl.ANY)
    _, total_rows = layout(rows, feat)
    inner_dp = 2
    outer_dp = ndp // inner_dp
    summed, final = pl.pallas_call(
        functools.partial(kernel, ndp, nmp),
        out_shape=(
            jax.ShapeDtypeStruct((total_rows, LANES), F32),
            jax.ShapeDtypeStruct((1, LANES), F32),
        ),
        in_specs=[hbm, vmem, vmem, hbm, hbm],
        out_specs=(vmem,) * 2,
        scratch_shapes=[
            pltpu.VMEM((images * patches, width), BF16),
            pltpu.VMEM((images, feat, patches), BF16),
            pltpu.VMEM((images, blocks, patches), jnp.int32),
            pltpu.VMEM((ndp - 1, rows, feat), BF16),
            pltpu.VMEM((width, featp), F32),
            pltpu.VMEM((feat, width), BF16),
            pltpu.VMEM((featp, LANES), F32),
            pltpu.VMEM((8, featp), F32),
            pltpu.VMEM((groups, 2 * GROUP, patches), F32),
            pltpu.VMEM((nmp - 1, groups, 2 * GROUP, patches), F32),
            pltpu.VMEM((images, patches), F32),
            pltpu.VMEM((images, patches), F32),
            pltpu.VMEM((images, patches), F32),
            pltpu.VMEM((feat, PAIR * patches), F32),
            pltpu.VMEM((feat, PAIR * patches), F32),
            pltpu.VMEM((feat, PAIR * patches), BF16),
            pltpu.VMEM((feat, PAIR * patches), BF16),
            pltpu.VMEM((featp, width), F32),
            pltpu.VMEM((featp, LANES), F32),
            pltpu.VMEM((CHUNK, patches), F32),
            pltpu.VMEM((inner_dp, outer_dp, total_rows, LANES), F32),
            pltpu.VMEM((outer_dp, total_rows, LANES), F32),
            pltpu.VMEM((outer_dp - 1, total_rows, LANES), F32),
            pltpu.VMEM((outer_dp - 1, total_rows, LANES), F32),
            pltpu.VMEM((1, LANES), F32),
            pltpu.VMEM((ntot - 1, 1, LANES), F32),
            dma((groups,)), dma((groups,)), dma(()),
            dma((ndp - 1,)), dma((ndp - 1,)),
            dma((nmp - 1, groups)), dma((nmp - 1, groups)),
            dma((outer_dp,)), dma((outer_dp,)),
            dma((outer_dp - 1,)), dma((outer_dp - 1,)),
            dma((ntot - 1,)), dma((ntot - 1,)),
        ],
        compiler_params=pltpu.CompilerParams(
            collective_id=0, has_side_effects=True, vmem_limit_bytes=60 * 1024 * 1024
        ),
    )(
        pred_input.reshape(images * patches, width),
        proj_weight,
        proj_bias.reshape(1, feat),
        jnp.swapaxes(targets, 1, 2),
        block_masks,
    )
    loss, clip, gw, gb = pl.pallas_call(
        functools.partial(finish, ndp, nmp),
        out_shape=(
            jax.ShapeDtypeStruct((1, 1), F32),
            jax.ShapeDtypeStruct((1, 1), F32),
            jax.ShapeDtypeStruct((rows, feat), F32),
            jax.ShapeDtypeStruct((1, feat), F32),
        ),
        in_specs=[vmem] * 2,
        out_specs=(vmem,) * 4,
    )(summed, final)
    return loss.reshape(()), clip.reshape(()), gw, gb.reshape(feat)


def solution(mesh):
    in_specs = (
        P("dp", None, None),
        P("dp", "mp"),
        P("mp"),
        P("dp", None, "mp"),
        P("dp", None, None),
    )
    out_specs = (P(), P(), P("dp", "mp"), P("mp"))
    return jax.shard_map(body, mesh=mesh, in_specs=in_specs, out_specs=out_specs, check_vma=False)
```

```python
import functools

import jax
import jax.numpy as jnp
from jax import lax
from jax.experimental import pallas as pl
from jax.experimental.pallas import tpu as pltpu
from jax.sharding import PartitionSpec as P

F32 = jnp.float32
BF16 = jnp.bfloat16
MESH = pl.DeviceIdType.MESH
LANES = 128
GROUP = 8
PAIR = 2
CHUNK = 16


def pad_to(n, m):
    return (n + m - 1) // m * m


def layout(rows, feat):
    starts, at = [], 0
    for _ in range(feat // LANES):
        starts.append(at)
        at += pad_to(rows, 8)
    if feat % LANES:
        starts.append(at)
        at += pad_to(rows // 2, 8)
    starts.append(at)
    return starts, at + 8


def finish(ndp, nmp, sum_ref, fin_ref, loss_ref, clip_ref, gw_ref, gb_ref):
    rows, feat = gw_ref.shape
    starts, _ = layout(rows, feat)
    tiles = pad_to(feat, LANES) // LANES
    count = sum_ref[starts[-1] + tiles + 1:starts[-1] + tiles + 2, 0:1]
    square, loss = fin_ref[:, 0:1], fin_ref[:, 1:2]
    norm = jnp.sqrt(square) / count
    scale = jnp.minimum(1.0, 1.0 / (norm + 1e-06))
    factor = scale / count
    loss_ref[...] = loss / count * (1.0 / (feat * nmp * ndp))
    clip_ref[...] = scale
    for n in range(feat // LANES):
        gw_ref[:, n * LANES:(n + 1) * LANES] = sum_ref[starts[n]:starts[n] + rows, :] * factor
    half = LANES // 2
    if feat % LANES:
        packed = sum_ref[starts[-2]:starts[-2] + rows // 2, :] * factor
        gw_ref[:rows // 2, feat - half:] = packed[:, :half]
        gw_ref[rows // 2:, feat - half:] = packed[:, half:]
    for n in range(tiles):
        stop = min((n + 1) * LANES, feat)
        bias = sum_ref[starts[-1] + n:starts[-1] + n + 1, :] * factor
        gb_ref[n * LANES:stop] = bias[0, :stop - n * LANES]


def kernel(ndp, nmp, x_hbm, w_ref, b_ref, t_hbm, m_hbm,
           out_ref, fin_ref,
           xv, tv, mv, wall, wfull, wt, bcol, brow, ssend, srecv, rbuf, mbuf, cbuf,
           pa, pb, sa, sb, acc, gacc, lacc, gsend, pairv, gmid, grecv, fsend, frecv,
           xsem, tsem, msem, wss, wrs, sss, srs, pss, prs, gss, grs, fss, frs):
    images, feat, patches = tv.shape
    width = xv.shape[1]
    rows = w_ref.shape[0]
    dp, mp = lax.axis_index("dp"), lax.axis_index("mp")
    inner_dp = gsend.shape[0]
    outer_dp = gsend.shape[1]
    near, far = lax.rem(dp, inner_dp), dp // inner_dp
    featp = acc.shape[0]
    groups = images // GROUP
    ntot = ndp * nmp
    me = dp * nmp + mp
    feat_full = feat * nmp

    def t_copy(g):
        s = pl.ds(g * GROUP, GROUP)
        return pltpu.make_async_copy(t_hbm.at[s], tv.at[s], tsem.at[g])

    def x_copy(g):
        s = pl.ds(g * GROUP * patches, GROUP * patches)
        return pltpu.make_async_copy(x_hbm.at[s], xv.at[s], xsem.at[g])

    m_copy = pltpu.make_async_copy(m_hbm, mv, msem)

    barrier = pltpu.get_barrier_semaphore()

    for g in range(groups):
        t_copy(g).start()
    m_copy.start()

    def greet(o, _):
        d = lax.rem(me + o, ntot)
        pl.semaphore_signal(barrier, inc=1, device_id=(d // nmp, lax.rem(d, nmp)), device_id_type=MESH)
        return 0

    lax.fori_loop(1, ntot, greet, 0)
    acc[...] = jnp.zeros_like(acc)
    gacc[...] = jnp.zeros_like(gacc)
    lacc[...] = jnp.zeros_like(lacc)
    sb[...] = jnp.zeros_like(sb)
    wfull[...] = jnp.zeros_like(wfull)
    brow[...] = jnp.zeros_like(brow)
    brow[0:1, :feat] = b_ref[...].reshape(1, feat)
    bcol[...] = jnp.transpose(jnp.broadcast_to(brow[0:1, :], (LANES, featp)))

    pl.semaphore_wait(barrier, ntot - 1)

    def w_copy(o):
        return pltpu.make_async_remote_copy(
            src_ref=w_ref, dst_ref=wall.at[o - 1], send_sem=wss.at[o - 1], recv_sem=wrs.at[o - 1],
            device_id=(lax.rem(dp + o, ndp), mp), device_id_type=MESH)

    for o in range(1, ndp):
        w_copy(o).start()

    def s_copy(o, g):
        return pltpu.make_async_remote_copy(
            src_ref=ssend.at[g], dst_ref=srecv.at[o - 1, g],
            send_sem=sss.at[o - 1, g], recv_sem=srs.at[o - 1, g],
            device_id=(dp, lax.rem(mp + o, nmp)), device_id_type=MESH)

    m_copy.wait()

    def cover(g, _):
        block = [jnp.sum(mv[g * GROUP + j], axis=0, keepdims=True) for j in range(GROUP)]
        cbuf[pl.ds(pl.multiple_of(g * GROUP, GROUP), GROUP), :] = jnp.concatenate(block, axis=0).astype(F32)
        return 0

    lax.fori_loop(0, groups, cover, 0)

    def stats(g, _):
        t_copy(g).wait()

        @pl.when(g >= 2)
        def _():
            x_copy(g - 2).start()

        sums, squares = [], []
        for j in range(GROUP):
            i = g * GROUP + j
            part = jnp.zeros((CHUNK, patches), F32)
            for c in range(0, feat, CHUNK):
                part = part + tv[i, c:c + CHUNK, :].astype(F32)
            total = jnp.sum(part, axis=0, keepdims=True)
            mean = total * (1.0 / feat)
            part = jnp.zeros((CHUNK, patches), F32)
            for c in range(0, feat, CHUNK):
                centred = tv[i, c:c + CHUNK, :].astype(F32) - mean
                part = part + centred * centred
            sums.append(total)
            squares.append(jnp.sum(part, axis=0, keepdims=True))
        ssend[g] = jnp.concatenate(sums + squares, axis=0)

        @pl.when(g > 0)
        def _():
            for o in range(1, nmp):
                s_copy(o, g - 1).start()

        return 0

    lax.fori_loop(0, groups, stats, 0)
    for g in range(groups - 2, groups):
        x_copy(g).start()

    def place(owner_static, block):
        wfull[owner_static * rows:(owner_static + 1) * rows, :feat] = block.astype(F32)

    for o in range(1, ndp):
        w_copy(o).wait_recv()
    for o in range(1, nmp):
        s_copy(o, groups - 1).start()
    for k in range(ndp):
        slot = lax.rem(dp - k + ndp, ndp)
        other = wall[jnp.maximum(slot - 1, 0)].astype(F32)
        mine = w_ref[...].astype(F32)
        place(k, jnp.where(slot == 0, mine, other))
    wt[...] = jnp.transpose(wfull[...])[:feat].astype(BF16)

    def x_rows(k):
        n = PAIR * patches
        return xv[pl.ds(pl.multiple_of(k * n, n), n), :]

    def project(p_ref, k):
        p_ref[...] = lax.dot_general(wt[...], x_rows(k), (((1,), (1,)), ((), ())), preferred_element_type=F32)

    def gradient(s_ref, k):
        acc[:feat, :] += jnp.dot(s_ref[...], x_rows(k), preferred_element_type=F32)

    def pointwise(p_ref, s_ref, k):
        img = k * PAIR
        rs = [rbuf[pl.ds(img + g, 1), :] for g in range(PAIR)]
        ms = [mbuf[pl.ds(img + g, 1), :] for g in range(PAIR)]
        cs = [cbuf[pl.ds(img + g, 1), :] for g in range(PAIR)]
        loss = jnp.zeros((CHUNK, patches), F32)
        for c in range(0, feat, CHUNK):
            bias = bcol[c:c + CHUNK, :]
            bias = jnp.concatenate([bias] * (patches // LANES), axis=1)
            total = jnp.zeros((CHUNK, LANES), F32)
            for g in range(PAIR):
                cols = slice(g * patches, (g + 1) * patches)
                t = tv[img + g, c:c + CHUNK, :].astype(F32)
                differ = (p_ref[c:c + CHUNK, cols] + bias) + (ms[g] - t * rs[g])
                clipped = jnp.clip(differ, -1.0, 1.0)
                source = clipped * cs[g]
                loss = loss + source * (differ - 0.5 * clipped)
                for h in range(0, patches, LANES):
                    total = total + source[:, h:h + LANES]
                s_ref[c:c + CHUNK, cols] = source.astype(BF16)
            gacc[c:c + CHUNK, :] += total
        lacc[...] += loss

    x_copy(0).wait()
    project(pa, 0)
    steps = images // PAIR
    per_group = GROUP // PAIR

    def outer(g, _):
        @pl.when(g + 1 < groups)
        def _():
            x_copy(g + 1).wait()

        for o in range(1, nmp):
            s_copy(o, g).wait_recv()
        parts = [ssend[g]] + [srecv[o - 1, g] for o in range(1, nmp)]
        sums = [p[:GROUP] for p in parts]
        mean = functools.reduce(jnp.add, sums) * (1.0 / feat_full)
        var = functools.reduce(jnp.add, [p[GROUP:] for p in parts])
        for s in sums:
            gap = s * (1.0 / feat) - mean
            var = var + feat * (gap * gap)
        rstd = lax.rsqrt(var * (1.0 / feat_full) + 1e-05)
        here = pl.ds(pl.multiple_of(g * GROUP, GROUP), GROUP)
        rbuf[here, :] = rstd
        mbuf[here, :] = mean * rstd

        def inner(j, _):
            k = g * per_group + 2 * j
            pointwise(pa, sa, k)
            project(pb, k + 1)
            gradient(sb, jnp.maximum(k - 1, 0))
            pointwise(pb, sb, k + 1)
            project(pa, jnp.minimum(k + 2, steps - 1))
            gradient(sa, k)
            return 0

        lax.fori_loop(0, per_group // 2, inner, 0)
        return 0

    lax.fori_loop(0, groups, outer, 0)
    gradient(sb, steps - 1)

    bias_part = jnp.sum(jnp.transpose(gacc[...]), axis=0, keepdims=True)
    loss_part = jnp.sum(lacc[...], keepdims=True)
    count_part = jnp.sum(cbuf[...], keepdims=True)
    at_row = lax.broadcasted_iota(jnp.int32, (8, LANES), 0)
    tiles = featp // LANES
    extra = jnp.where(at_row == tiles, loss_part, count_part)
    for n in range(tiles):
        extra = jnp.where(at_row == n, bias_part[:, n * LANES:(n + 1) * LANES], extra)
    starts, total_rows = layout(rows, feat)
    full = jnp.transpose(acc[...])
    for k in range(ndp):
        slot = gsend.at[k % inner_dp, k // inner_dp]
        if rows % 16:
            slot[...] = jnp.zeros(slot.shape, F32)
        mine = full[k * rows:(k + 1) * rows]
        for n in range(feat // LANES):
            slot[starts[n]:starts[n] + rows, :] = mine[:, n * LANES:(n + 1) * LANES]
        if feat % LANES:
            slot[starts[-2]:starts[-2] + rows // 2, :] = jnp.concatenate(
                [mine[:rows // 2, feat - LANES // 2:feat], mine[rows // 2:, feat - LANES // 2:feat]], axis=1)
        slot[starts[-1]:, :] = extra

    other = 1 - near

    def p_copy(o):
        to = lax.rem(far + o, outer_dp)
        return pltpu.make_async_remote_copy(
            src_ref=gsend.at[other, to], dst_ref=pairv.at[o], send_sem=pss.at[o], recv_sem=prs.at[o],
            device_id=(far * inner_dp + other, mp), device_id_type=MESH)

    def g_copy(o):
        to = lax.rem(far + o, outer_dp)
        return pltpu.make_async_remote_copy(
            src_ref=gmid.at[o - 1], dst_ref=grecv.at[o - 1], send_sem=gss.at[o - 1], recv_sem=grs.at[o - 1],
            device_id=(to * inner_dp + near, mp), device_id_type=MESH)

    order = list(range(1, outer_dp)) + [0]
    for o in order:
        p_copy(o).start()
    for o in order:
        p_copy(o).wait_recv()
        pair = gsend[near, lax.rem(far + o, outer_dp)] + pairv[o]
        if o:
            gmid[o - 1] = pair
            g_copy(o).start()
    for o in range(1, outer_dp):
        g_copy(o).wait_recv()
        pair = pair + grecv[o - 1]
    out_ref[...] = pair
    grad = pair[:starts[-1]]
    sums = pair[starts[-1]:]
    bias_grad = sums[:tiles]
    square = jnp.sum(grad * grad, keepdims=True)
    bias_square = jnp.sum(bias_grad * bias_grad, keepdims=True)
    lane = lax.broadcasted_iota(jnp.int32, (1, LANES), 1)
    fsend[...] = jnp.where(lane == 0, square + bias_square * (1.0 / ndp), sums[tiles:tiles + 1, :])

    def f_copy(o):
        d = lax.rem(me + o, ntot)
        return pltpu.make_async_remote_copy(
            src_ref=fsend, dst_ref=frecv.at[o - 1], send_sem=fss.at[o - 1], recv_sem=frs.at[o - 1],
            device_id=(d // nmp, lax.rem(d, nmp)), device_id_type=MESH)

    def f_start(o, _):
        f_copy(o).start()
        return 0

    def f_wait(o, _):
        f_copy(o).wait_recv()
        return 0

    lax.fori_loop(1, ntot, f_start, 0)
    lax.fori_loop(1, ntot, f_wait, 0)
    fin_ref[...] = fsend[...] + jnp.sum(frecv[...], axis=0)

    for o in range(1, ndp):
        w_copy(o).wait_send()
    for o in order:
        p_copy(o).wait_send()
        if o:
            g_copy(o).wait_send()

    def s_drain(g, _):
        for o in range(1, nmp):
            s_copy(o, g).wait_send()
        return 0

    def f_drain(o, _):
        f_copy(o).wait_send()
        return 0

    lax.fori_loop(0, groups, s_drain, 0)
    lax.fori_loop(1, ntot, f_drain, 0)


def body(pred_input, proj_weight, proj_bias, targets, block_masks):
    images, patches, width = pred_input.shape
    feat = targets.shape[2]
    rows = proj_weight.shape[0]
    blocks = block_masks.shape[1]
    ndp, nmp = lax.axis_size("dp"), lax.axis_size("mp")
    ntot = ndp * nmp
    featp = pad_to(feat, LANES)
    groups = images // GROUP
    dma = pltpu.SemaphoreType.DMA
    vmem = pl.BlockSpec(memory_space=pltpu.VMEM)
    hbm = pl.BlockSpec(memory_space=pl.ANY)
    _, total_rows = layout(rows, feat)
    inner_dp = 2
    outer_dp = ndp // inner_dp
    summed, final = pl.pallas_call(
        functools.partial(kernel, ndp, nmp),
        out_shape=(
            jax.ShapeDtypeStruct((total_rows, LANES), F32),
            jax.ShapeDtypeStruct((1, LANES), F32),
        ),
        in_specs=[hbm, vmem, vmem, hbm, hbm],
        out_specs=(vmem,) * 2,
        scratch_shapes=[
            pltpu.VMEM((images * patches, width), BF16),
            pltpu.VMEM((images, feat, patches), BF16),
            pltpu.VMEM((images, blocks, patches), jnp.int32),
            pltpu.VMEM((ndp - 1, rows, feat), BF16),
            pltpu.VMEM((width, featp), F32),
            pltpu.VMEM((feat, width), BF16),
            pltpu.VMEM((featp, LANES), F32),
            pltpu.VMEM((8, featp), F32),
            pltpu.VMEM((groups, 2 * GROUP, patches), F32),
            pltpu.VMEM((nmp - 1, groups, 2 * GROUP, patches), F32),
            pltpu.VMEM((images, patches), F32),
            pltpu.VMEM((images, patches), F32),
            pltpu.VMEM((images, patches), F32),
            pltpu.VMEM((feat, PAIR * patches), F32),
            pltpu.VMEM((feat, PAIR * patches), F32),
            pltpu.VMEM((feat, PAIR * patches), BF16),
            pltpu.VMEM((feat, PAIR * patches), BF16),
            pltpu.VMEM((featp, width), F32),
            pltpu.VMEM((featp, LANES), F32),
            pltpu.VMEM((CHUNK, patches), F32),
            pltpu.VMEM((inner_dp, outer_dp, total_rows, LANES), F32),
            pltpu.VMEM((outer_dp, total_rows, LANES), F32),
            pltpu.VMEM((outer_dp - 1, total_rows, LANES), F32),
            pltpu.VMEM((outer_dp - 1, total_rows, LANES), F32),
            pltpu.VMEM((1, LANES), F32),
            pltpu.VMEM((ntot - 1, 1, LANES), F32),
            dma((groups,)), dma((groups,)), dma(()),
            dma((ndp - 1,)), dma((ndp - 1,)),
            dma((nmp - 1, groups)), dma((nmp - 1, groups)),
            dma((outer_dp,)), dma((outer_dp,)),
            dma((outer_dp - 1,)), dma((outer_dp - 1,)),
            dma((ntot - 1,)), dma((ntot - 1,)),
        ],
        compiler_params=pltpu.CompilerParams(
            collective_id=0, has_side_effects=True, vmem_limit_bytes=60 * 1024 * 1024
        ),
    )(
        pred_input.reshape(images * patches, width),
        proj_weight,
        proj_bias,
        jnp.swapaxes(targets, 1, 2),
        block_masks,
    )
    loss, clip, gw, gb = pl.pallas_call(
        functools.partial(finish, ndp, nmp),
        out_shape=(
            jax.ShapeDtypeStruct((1, 1), F32),
            jax.ShapeDtypeStruct((1, 1), F32),
            jax.ShapeDtypeStruct((rows, feat), F32),
            jax.ShapeDtypeStruct((feat,), F32),
        ),
        in_specs=[vmem] * 2,
        out_specs=(vmem,) * 4,
    )(summed, final)
    return loss.reshape(()), clip.reshape(()), gw, gb


def solution(mesh):
    in_specs = (
        P("dp", None, None),
        P("dp", "mp"),
        P("mp"),
        P("dp", None, "mp"),
        P("dp", None, None),
    )
    out_specs = (P(), P(), P("dp", "mp"), P("mp"))
    return jax.shard_map(body, mesh=mesh, in_specs=in_specs, out_specs=out_specs, check_vma=False)
```
